32 devices in a mesh: groups: 2 (over y), blk: 16 (over z, x, core).
Axes of the slice: x: 2, y: 2, z: 4, core: 2. Of those that a mesh axis runs over, the one named last changes fastest.
Arguments:
- basis: float32 [8, 64, 480, 128], P(None, ('groups', 'blk')), parts along dimension 1
- nbr_block: int32 [64, 14], P(('groups', 'blk')), parts along dimension 0, may hold values from 0 to 31, as said below
- nbr_type: int32 [64, 14], P(('groups', 'blk')), parts along dimension 0, may hold values from 0 to 7
- nbr_count: int32 [64], P(('groups', 'blk')), parts along dimension 0, may hold values from 2 to 14, as said below
- sphere_type: int32 [64, 128], P(('groups', 'blk')), parts along dimension 0, may hold values from 0 to 3
- trans: float32 [8, 480, 480], replicated, may hold values from -0.25 to 0.25
- coup: float32 [8, 128, 128], replicated, may hold values from -0.5 to 0.5
- tmat: float32 [4, 480, 480], replicated, may hold values from -0.125 to 0.125
Outputs:
- new_vectors: float32 [2, 64, 480, 128], P(None, ('groups', 'blk')), parts along dimension 1
- hess_first: float32 [18], P('groups'), parts along dimension 0
- hess_second: float32 [20], P('groups'), parts along dimension 0
The draws below stay inside these ranges and needn't reach their ends.
There are 2 independent parts, one for each index of `groups`. The reference program is written for one: setup_inputs(seed, part) draws one part's arguments, and reference() takes and returns one part's arrays. A program takes and returns all parts, laid end to end along the dimension named above; an argument that names none is the same for every part. Nothing has to cross between parts.
Inputs may be any that keep to these rules, and one draw needn't show every extreme that they name: `nbr_block`: each entry lies within 2 blocks of its own block; a block may be near itself. The first two slots of block b hold, in either order, the blocks b - 2 and b + 2, clipped to the cluster. Block b uses the first nbr_count[b] slots of its lists; some run of blocks uses all 14.
All inputs are finite; a program needn't handle non-finite values.
Results may differ from the reference program's by a relative error of at most 0.0003.
Values sent between devices are 32-bit elements; how exact they have to be, the bound alone decides.
A program may use at most 128 MiB of HBM per device.

```python
import jax
import jax.numpy as jnp
from jax import lax

COEF = 480
SPB = 128
BLK_DEV = 2
NBR = 14
NTYPE = 8
NSTYPE = 4
KRY = 8
RADIUS = 2
NBLOCKS = 32


def draw_basis(key, part):
    common = jax.random.normal(jax.random.fold_in(key, 1), (NBLOCKS, COEF, SPB), jnp.float32)
    strength = jax.random.uniform(jax.random.fold_in(key, 2), (KRY,), jnp.float32, 0.5, 1.0)
    position = jnp.arange(NBLOCKS, dtype=jnp.float32) / float(max(NBLOCKS - 1, 1))
    rough_part = jax.random.normal(jax.random.fold_in(key, 3), (KRY, NBLOCKS, COEF, SPB), jnp.float32)
    ramp_scale = 0.5 + position
    return strength[:, None, None, None] * ramp_scale[None, :, None, None] * common[None] + rough_part


def draw_nbr_block(key, part):
    offsets = jax.random.randint(jax.random.fold_in(key, 11), (NBLOCKS, NBR), -RADIUS, RADIUS + 1)
    flipped = jax.random.randint(jax.random.fold_in(key, 12), (NBLOCKS,), 0, 2)
    lower_first = jnp.where(flipped == 0, -RADIUS, RADIUS)
    slot_index = jnp.arange(NBR, dtype=jnp.int32)[None, :]
    offsets = jnp.where(slot_index == 0, lower_first[:, None], offsets)
    offsets = jnp.where(slot_index == 1, -lower_first[:, None], offsets)
    base_rows = jnp.arange(NBLOCKS, dtype=jnp.int32)[:, None]
    return jnp.clip(base_rows + offsets, 0, NBLOCKS - 1).astype(jnp.int32)


def draw_nbr_count(key, part):
    center = jax.random.randint(jax.random.fold_in(key, 21), (), 0, NBLOCKS)
    light_count = jax.random.randint(jax.random.fold_in(key, 22), (NBLOCKS,), 2, NBR // 2 + 2)
    light_count = jnp.minimum(light_count, NBR)
    block_rows = jnp.arange(NBLOCKS, dtype=jnp.int32)
    dense_run = jnp.abs(block_rows - center) < 2 * BLK_DEV
    return jnp.where(dense_run, NBR, light_count).astype(jnp.int32)


def set_ends(drawn, rng, low, high):
    longest = drawn.shape.index(max(drawn.shape))
    spots = []
    for shift in (0, 1):
        where = [jax.random.randint(jax.random.fold_in(rng, axis), (), 0, length) for axis, length in enumerate(drawn.shape)]
        where[longest] = (where[longest] + shift) % drawn.shape[longest]
        spots.append(tuple(where))
    return drawn.at[spots[0]].set(low).at[spots[1]].set(high)


def scatter_about(stream_key, shape, spread, reach, held_as=jnp.bfloat16):
    array = jax.random.normal(stream_key, shape, jnp.float32) * spread
    return jnp.minimum(jnp.maximum(array, -reach), reach).astype(held_as)


def setup_inputs(seed: int = 0, part: int = 0) -> dict:
    streams_of = jax.random.split(jax.random.key(seed), 9)
    own_keys = jax.random.split(jax.random.fold_in(streams_of[8], part), 9)
    return {
        "basis": draw_basis(jax.random.fold_in(jax.random.fold_in(streams_of[8], part), 71), part),
        "nbr_block": draw_nbr_block(jax.random.fold_in(jax.random.fold_in(streams_of[8], part), 71), part),
        "nbr_type": set_ends(jax.random.randint(own_keys[2], (NBLOCKS, NBR), 0, NTYPE), jax.random.fold_in(own_keys[2], 1), 0, NTYPE - 1).astype(jnp.int32),
        "nbr_count": draw_nbr_count(jax.random.fold_in(jax.random.fold_in(streams_of[8], part), 71), part),
        "sphere_type": set_ends(jax.random.randint(own_keys[4], (NBLOCKS, SPB), 0, NSTYPE), jax.random.fold_in(own_keys[4], 1), 0, NSTYPE - 1).astype(jnp.int32),
        "trans": scatter_about(streams_of[5], (NTYPE, COEF, COEF), COEF ** -0.5, 0.25, jnp.float32),
        "coup": scatter_about(streams_of[6], (NTYPE, SPB, SPB), SPB ** -0.5, 0.5, jnp.float32),
        "tmat": scatter_about(streams_of[7], (NSTYPE, COEF, COEF), (4 * COEF) ** -0.5, 0.125, jnp.float32),
    }


def operator_apply(vector, nbr_block, nbr_type, nbr_count, sphere_type, trans, coup, tmat):

    def block_image(items):
        near_ids, pair_kinds, live_count, sphere_kinds = items
        sources = vector[near_ids]
        moved = jnp.einsum('kij,kjs->kis', trans[pair_kinds], sources, precision=lax.Precision.HIGHEST)
        coupled = jnp.einsum('kis,kts->kit', moved, coup[pair_kinds], precision=lax.Precision.HIGHEST)
        active = (jnp.arange(NBR, dtype=jnp.int32) < live_count).astype(jnp.float32)
        summed = lax.optimization_barrier(jnp.sum(active[:, None, None] * coupled, axis=0))
        scattered = jnp.einsum('tij,js->tis', tmat, summed, precision=lax.Precision.HIGHEST)
        onehot = (sphere_kinds[None, :] == jnp.arange(NSTYPE, dtype=jnp.int32)[:, None]).astype(jnp.float32)
        return lax.optimization_barrier(jnp.sum(onehot[:, None, :] * scattered, axis=0))
    images = lax.map(block_image, (nbr_block, nbr_type, nbr_count, sphere_type))
    return vector - images

def arnoldi(vectors, vector, tables):
    image = operator_apply(vector, *tables)
    total_cells = float(NBLOCKS * COEF * SPB)
    coeffs = jnp.einsum('kbcs,bcs->k', vectors, image, precision=lax.Precision.HIGHEST) / total_cells
    remainder = image - jnp.einsum('k,kbcs->bcs', coeffs, vectors, precision=lax.Precision.HIGHEST)
    norm_value = jnp.sqrt(jnp.sum(remainder * remainder) / total_cells + 1e-06)
    return (remainder / norm_value, jnp.concatenate([coeffs, norm_value[None]]))

def reference(basis, nbr_block, nbr_type, nbr_count, sphere_type, trans, coup, tmat):
    tables = (nbr_block, nbr_type, nbr_count, sphere_type, trans, coup, tmat)
    first_new, hess_first = arnoldi(basis, basis[KRY - 1], tables)
    extended = jnp.concatenate([basis, first_new[None]], axis=0)
    second_new, hess_second = arnoldi(extended, first_new, tables)
    return (jnp.stack([first_new, second_new]), hess_first, hess_second)
```

```python
import functools

import jax
import jax.numpy as jnp
from jax import lax
from jax.experimental import pallas as pl
from jax.experimental.pallas import tpu as pltpu
from jax.sharding import PartitionSpec as P

F32 = jnp.float32
BF16 = jnp.bfloat16
REACH = 2
MESH = pl.DeviceIdType.MESH


def split(x):
    hi = x.astype(BF16)
    return hi, (x - hi.astype(F32)).astype(BF16)


def mm(a, b):
    return jnp.dot(a, b, preferred_element_type=F32)


def kernel(
    n, dims, w_ref, stype, basis, trans, coup, tmat, out, hess,
    bv, stage, mstage, cstage, thi, tlo, mhi, mlo, rct, halo1, halo2,
    za_hi, za_lo, zb_hi, zb_lo, acc, wbuf, fbuf, gbuf, send1, send2, slots1, slots2,
    lsem, ssem, rsem, hsend, hrecv, osem,
):
    kry, nb, coef, spb, kinds, skinds, cpad = dims
    window = 3 * nb
    me = lax.axis_index("blk")
    cells = float(n * nb * coef * spb)

    loads = [pltpu.make_async_copy(basis.at[kry - 1], bv.at[kry - 1], lsem.at[0])]
    loads.append(pltpu.make_async_copy(coup, cstage, lsem.at[1]))
    tl = [pltpu.make_async_copy(trans.at[t], stage.at[t], lsem.at[2 + t]) for t in range(kinds)]
    bl = pltpu.make_async_copy(
        basis.at[pl.ds(0, kry - 1)], bv.at[pl.ds(0, kry - 1)], lsem.at[2 + kinds]
    )
    ml_ = [
        pltpu.make_async_copy(tmat.at[t], mstage.at[t], lsem.at[3 + kinds + t])
        for t in range(skinds)
    ]
    for c in loads + tl + [bl] + ml_:
        c.start()

    barrier = pltpu.get_barrier_semaphore()

    def greet(d, _):
        pl.semaphore_signal(
            barrier, inc=1, device_id={"blk": lax.rem(me + d, n)}, device_id_type=MESH
        )
        return 0

    lax.fori_loop(1, n, greet, 0)
    pl.semaphore_wait(barrier, n - 1)

    def halo_copy(src, halo, step, side):
        peer = jnp.minimum(me + 1, n - 1) if side == 0 else jnp.maximum(me - 1, 0)
        return pltpu.make_async_remote_copy(
            src_ref=src,
            dst_ref=halo.at[side],
            send_sem=hsend.at[2 * step + side],
            recv_sem=hrecv.at[2 * step + side],
            device_id={"blk": peer},
            device_id_type=MESH,
        )

    def halo_start(src, halo, step):
        @pl.when(me < n - 1)
        def _():
            halo_copy(src, halo, step, 0).start()

        @pl.when(me > 0)
        def _():
            halo_copy(src, halo, step, 1).start()

    def halo_wait(src, halo, step):
        @pl.when(me < n - 1)
        def _():
            halo_copy(src, halo, step, 0).wait_send()
            halo_copy(src, halo, step, 1).wait_recv()

        @pl.when(me > 0)
        def _():
            halo_copy(src, halo, step, 1).wait_send()
            halo_copy(src, halo, step, 0).wait_recv()

    halo_start(basis.at[kry - 1], halo1, 0)

    @pl.when(me == 0)
    def _():
        halo1[0] = jnp.zeros(halo1.shape[1:], F32)
        halo2[0] = jnp.zeros(halo2.shape[1:], F32)

    @pl.when(me == n - 1)
    def _():
        halo1[1] = jnp.zeros(halo1.shape[1:], F32)
        halo2[1] = jnp.zeros(halo2.shape[1:], F32)

    tail = (coef // 128) * 128
    if cpad > coef:
        for z in (za_hi, za_lo, zb_hi, zb_lo):
            z[coef:, :] = jnp.zeros((cpad - coef, z.shape[1]), BF16)

    loads[1].wait()
    for t in range(kinds):
        ch, cl = split(cstage[t])
        rct[t, :spb, :spb] = ch
        rct[t, :spb, spb:] = ch
        rct[t, spb:, :spb] = cl
        rct[t, spb:, spb:] = cl

    def prepare(src, hi_ref, lo_ref, count):
        def one(t, _):
            hi, lo = split(src[t])
            if cpad > coef:
                hi_ref[t, :, tail:] = jnp.zeros((coef, cpad - tail), BF16)
                lo_ref[t, :, tail:] = jnp.zeros((coef, cpad - tail), BF16)
            hi_ref[t, :, :coef] = hi
            lo_ref[t, :, :coef] = lo
            return 0

        lax.fori_loop(0, count, one, 0)

    for c in tl:
        c.wait()
    prepare(stage, thi, tlo, kinds)
    loads[0].wait()
    bl.wait()

    pairs = [(i, j) for i in range(kry) for j in range(i, kry)]
    groups = coef // 8

    def sums(count, terms, b_count=nb):
        def row(r, carry):
            at = pl.ds(pl.multiple_of(r * 8, 8), 8)
            for b in range(b_count):
                new = terms(b, at)
                carry = tuple(x + y for x, y in zip(carry, new))
            return carry

        return lax.fori_loop(0, groups, row, (jnp.zeros((8, 128), F32),) * count)

    def gram_terms(b, at):
        vs = [bv[i, b, at, :] for i in range(kry)]
        return [vs[i] * vs[j] for i, j in pairs]

    gram = sums(len(pairs), gram_terms)
    gbuf[...] = jnp.concatenate(
        [jnp.sum(g, axis=0, keepdims=True) for g in gram]
        + [jnp.zeros((gbuf.shape[0] - len(pairs), 128), F32)],
        axis=0,
    )
    for c in ml_:
        c.wait()
    prepare(mstage, mhi, mlo, skinds)

    def operator_apply(vec, halo):
        def source(p):
            if p < nb:
                return halo[0, p]
            if p < 2 * nb:
                return vec[p - nb]
            return halo[1, p - 2 * nb]

        def couple(t, hi_ref, lo_ref):
            for b in range(nb):
                m = None
                for p in range(nb + b - REACH, nb + b + REACH + 1):
                    term = w_ref[(b * kinds + t) * window + p] * source(p)
                    m = term if m is None else m + term
                mh, ml = split(m)
                r = lax.dot_general(
                    jnp.concatenate([mh, ml], axis=1),
                    rct[t],
                    (((1,), (1,)), ((), ())),
                    preferred_element_type=F32,
                )
                zh, zl = split(r[:, :spb] + r[:, spb:])
                hi_ref[:coef, b * spb : (b + 1) * spb] = zh
                lo_ref[:coef, b * spb : (b + 1) * spb] = zl

        def move(t, hi_ref, lo_ref):
            hi = hi_ref[...]
            acc[...] += mm(thi[t], hi) + mm(thi[t], lo_ref[...]) + mm(tlo[t], hi)

        acc[...] = jnp.zeros(acc.shape, F32)
        couple(0, za_hi, za_lo)

        def two(u, _):
            move(2 * u, za_hi, za_lo)
            couple(2 * u + 1, zb_hi, zb_lo)
            move(2 * u + 1, zb_hi, zb_lo)
            couple(jnp.minimum(2 * u + 2, kinds - 1), za_hi, za_lo)
            return 0

        lax.fori_loop(0, kinds // 2, two, 0)
        sh, sl = split(acc[...])
        za_hi[:coef, :] = sh
        za_lo[:coef, :] = sl
        acc[...] = jnp.concatenate([vec[b] for b in range(nb)], axis=1)
        kind_row = jnp.concatenate([stype[b : b + 1, :] for b in range(nb)], axis=1)

        def scatter(t, _):
            hi = za_hi[...]
            y = mm(mhi[t], hi) + mm(mhi[t], za_lo[...]) + mm(mlo[t], hi)
            mask = (kind_row == t).astype(F32)
            acc[...] -= mask * y
            return 0

        lax.fori_loop(0, skinds, scatter, 0)
        for b in range(nb):
            wbuf[b] = acc[:, b * spb : (b + 1) * spb]

    lane = lax.broadcasted_iota(jnp.int32, (8, 128), 1)

    def allreduce(step, rows, send, slots):
        k = rows.shape[0]
        tot = jnp.sum(rows, axis=1, keepdims=True)
        here = lax.broadcasted_iota(jnp.int32, (k, 128), 1) == lax.broadcasted_iota(
            jnp.int32, (k, 128), 0
        )
        packed = jnp.sum(jnp.where(here, tot, 0.0), axis=0, keepdims=True)
        packed = jnp.broadcast_to(packed, (8, 128))
        send[...] = packed
        slots[me] = packed

        def copy(d, slot, peer):
            return pltpu.make_async_remote_copy(
                src_ref=send,
                dst_ref=slots.at[slot],
                send_sem=ssem.at[step, d],
                recv_sem=rsem.at[step, slot],
                device_id={"blk": peer},
                device_id_type=MESH,
            )

        def go(d, _):
            copy(d, me, lax.rem(me + d, n)).start()
            return 0

        def done(d, _):
            peer = lax.rem(me + d, n)
            c = copy(d, peer, peer)
            c.wait_send()
            c.wait_recv()
            return 0

        lax.fori_loop(1, n, go, 0)
        lax.fori_loop(1, n, done, 0)
        total = jnp.sum(slots[...], axis=0)
        return lambda i: jnp.sum(jnp.where(lane == i, total, 0.0), axis=1, keepdims=True)

    def pack(parts, more):
        rows = [jnp.sum(x, axis=0, keepdims=True) for x in parts]
        pad = (-len(rows)) % 8
        rows += [jnp.zeros((1, 128), F32)] * pad
        head = jnp.concatenate(rows, axis=0)
        return (head if more is None else jnp.concatenate([head, more], axis=0)), len(rows)

    def norm(count, proj, image_sq, gram_of):
        coeffs = [x / cells for x in proj]
        squares = image_sq
        for i in range(count):
            inner = None
            for j in range(count):
                term = gram_of(i, j) * coeffs[j]
                inner = term if inner is None else inner + term
            squares = squares + coeffs[i] * (inner - 2.0 * proj[i])
        return coeffs, jnp.sqrt(squares / cells + 1e-06)

    def hess_row(coeffs, beta):
        row = jnp.zeros((8, 128), F32)
        for i, c in enumerate(coeffs + [beta]):
            row = jnp.where(lane == i, c, row)
        return row

    halo_wait(basis.at[kry - 1], halo1, 0)
    operator_apply(bv.at[kry - 1], halo1)

    def proj_terms1(b, at):
        w = wbuf[b, at, :]
        return [w * bv[i, b, at, :] for i in range(kry)] + [w * w]

    rows, base = pack(sums(kry + 1, proj_terms1), gbuf[...])
    get1 = allreduce(0, rows, send1, slots1)
    gram8 = {}
    for k, (i, j) in enumerate(pairs):
        gram8[i, j] = gram8[j, i] = get1(base + k)
    h1, beta1 = norm(kry, [get1(i) for i in range(kry)], get1(kry), lambda i, j: gram8[i, j])
    hess[0] = hess_row(h1, beta1)
    inv1 = 1.0 / beta1

    def first_terms(b, at):
        f = wbuf[b, at, :]
        vs = [bv[i, b, at, :] for i in range(kry)]
        for i in range(kry):
            f = f - h1[i] * vs[i]
        f = f * inv1
        fbuf[0, b, at, :] = f
        return [f * v for v in vs] + [f * f]

    extra = sums(kry + 1, first_terms)
    halo_start(fbuf.at[0], halo2, 1)
    first_out = pltpu.make_async_copy(fbuf.at[0], out.at[0], osem.at[0])
    first_out.start()

    halo_wait(fbuf.at[0], halo2, 1)
    operator_apply(fbuf.at[0], halo2)

    def proj_terms2(b, at):
        w = wbuf[b, at, :]
        return [w * bv[i, b, at, :] for i in range(kry)] + [w * fbuf[0, b, at, :], w * w]

    rows, _ = pack(tuple(sums(kry + 2, proj_terms2)) + tuple(extra), None)
    get2 = allreduce(1, rows, send2, slots2)
    gram9 = dict(gram8)
    for i in range(kry + 1):
        gram9[i, kry] = gram9[kry, i] = get2(kry + 2 + i)
    h2, beta2 = norm(
        kry + 1, [get2(i) for i in range(kry + 1)], get2(kry + 1), lambda i, j: gram9[i, j]
    )
    hess[1] = hess_row(h2, beta2)
    inv2 = 1.0 / beta2

    def second(r, _):
        at = pl.ds(pl.multiple_of(r * 8, 8), 8)
        for b in range(nb):
            f = wbuf[b, at, :]
            for i in range(kry):
                f = f - h2[i] * bv[i, b, at, :]
            f = f - h2[kry] * fbuf[0, b, at, :]
            fbuf[1, b, at, :] = f * inv2
        return 0

    lax.fori_loop(0, groups, second, 0)
    second_out = pltpu.make_async_copy(fbuf.at[1], out.at[1], osem.at[1])
    second_out.start()
    first_out.wait()
    second_out.wait()


def shards(n, basis, nbr_block, nbr_type, nbr_count, sphere_type, trans, coup, tmat):
    kry, nb, coef, spb = basis.shape
    kinds, skinds = trans.shape[0], tmat.shape[0]
    cpad = -(-coef // 128) * 128
    window = 3 * nb
    rows = nbr_block - lax.axis_index("blk") * nb + nb
    live = jnp.arange(nbr_block.shape[1], dtype=jnp.int32)[None, :] < nbr_count[:, None]
    code = jnp.where(live, nbr_type * window + rows, -1)
    weights = jnp.sum(
        (code[:, None, :] == jnp.arange(kinds * window, dtype=jnp.int32)[None, :, None]).astype(F32),
        axis=2,
    ).reshape(-1)
    npairs = kry * (kry + 1) // 2
    any_ = pl.BlockSpec(memory_space=pl.ANY)
    vm = pl.BlockSpec(memory_space=pltpu.VMEM)
    wide = nb * spb
    out, hess = pl.pallas_call(
        functools.partial(kernel, n, (kry, nb, coef, spb, kinds, skinds, cpad)),
        out_shape=(
            jax.ShapeDtypeStruct((2, nb, coef, spb), F32),
            jax.ShapeDtypeStruct((2, 8, 128), F32),
        ),
        in_specs=[pl.BlockSpec(memory_space=pltpu.SMEM), vm, any_, any_, any_, any_],
        out_specs=(any_, vm),
        scratch_shapes=[
            pltpu.VMEM((kry, nb, coef, spb), F32),
            pltpu.VMEM((kinds, coef, coef), F32),
            pltpu.VMEM((skinds, coef, coef), F32),
            pltpu.VMEM((kinds, spb, spb), F32),
            pltpu.VMEM((kinds, coef, cpad), BF16),
            pltpu.VMEM((kinds, coef, cpad), BF16),
            pltpu.VMEM((skinds, coef, cpad), BF16),
            pltpu.VMEM((skinds, coef, cpad), BF16),
            pltpu.VMEM((kinds, 2 * spb, 2 * spb), BF16),
            pltpu.VMEM((2, nb, coef, spb), F32),
            pltpu.VMEM((2, nb, coef, spb), F32),
        ]
        + [pltpu.VMEM((cpad, wide), BF16)] * 4
        + [
            pltpu.VMEM((coef, wide), F32),
            pltpu.VMEM((nb, coef, spb), F32),
            pltpu.VMEM((2, nb, coef, spb), F32),
            pltpu.VMEM((-(-npairs // 8) * 8, 128), F32),
            pltpu.VMEM((8, 128), F32),
            pltpu.VMEM((8, 128), F32),
            pltpu.VMEM((n, 8, 128), F32),
            pltpu.VMEM((n, 8, 128), F32),
            pltpu.SemaphoreType.DMA((3 + kinds + skinds,)),
            pltpu.SemaphoreType.DMA((2, n)),
            pltpu.SemaphoreType.DMA((2, n)),
            pltpu.SemaphoreType.DMA((4,)),
            pltpu.SemaphoreType.DMA((4,)),
            pltpu.SemaphoreType.DMA((2,)),
        ],
        compiler_params=pltpu.CompilerParams(
            collective_id=0, has_side_effects=True, vmem_limit_bytes=60 * 1024 * 1024
        ),
    )(weights, sphere_type, basis, trans, coup, tmat)
    return out, hess[0, 0, : kry + 1], hess[1, 0, : kry + 2]


def solution(mesh):
    return jax.shard_map(
        functools.partial(shards, mesh.shape["blk"]),
        mesh=mesh,
        in_specs=(
            P(None, ("groups", "blk"), None, None),
            P(("groups", "blk"), None),
            P(("groups", "blk"), None),
            P(("groups", "blk")),
            P(("groups", "blk"), None),
            P(),
            P(),
            P(),
        ),
        out_specs=(P(None, ("groups", "blk"), None, None), P("groups"), P("groups")),
        check_vma=False,
    )
```

```python
import functools

import jax
import jax.numpy as jnp
from jax import lax
from jax.experimental import pallas as pl
from jax.experimental.pallas import tpu as pltpu
from jax.sharding import PartitionSpec as P

F32 = jnp.float32
BF16 = jnp.bfloat16
REACH = 2
CHUNK = 128
MESH = pl.DeviceIdType.MESH


def split(x):
    hi = x.astype(BF16)
    return hi, (x - hi.astype(F32)).astype(BF16)


def factors(n):
    near = max(f for f in range(1, n + 1) if n % f == 0 and f * f <= n)
    return near, n // near


def mm(a, b):
    return jnp.dot(a, b, preferred_element_type=F32)


def kernel(
    n, dims, w_ref, stype, basis, trans, coup, tmat, out, hess,
    bv, stage, mstage, cstage, thi, tlo, mhi, mlo, rct, halo1, halo2,
    za_hi, za_lo, zb_hi, zb_lo, sh_ref, sl_ref, acc, wbuf, fbuf, gbuf,
    send, slots_a, slots_b, lsem, ssem, ra_sem, rb_sem, hsend, hrecv, osem,
):
    kry, nb, coef, spb, kinds, skinds, cpad = dims
    window = 3 * nb
    me = lax.axis_index("blk")
    cells = float(n * nb * coef * spb)
    near, far = factors(n)
    chunks = [(c, min(CHUNK, coef - c)) for c in range(0, coef, CHUNK)]
    my_far, my_near = lax.div(me, near), lax.rem(me, near)

    def near_peer(d):
        return my_far * near + lax.rem(my_near + d, near)

    def far_peer(d):
        return lax.rem(my_far + d, far) * near + my_near

    loads = [pltpu.make_async_copy(basis.at[kry - 1], bv.at[kry - 1], lsem.at[0])]
    loads.append(pltpu.make_async_copy(coup, cstage, lsem.at[1]))
    tl = [pltpu.make_async_copy(trans.at[t], stage.at[t], lsem.at[2 + t]) for t in range(kinds)]
    bl = pltpu.make_async_copy(
        basis.at[pl.ds(0, kry - 1)], bv.at[pl.ds(0, kry - 1)], lsem.at[2 + kinds]
    )
    ml_ = [
        pltpu.make_async_copy(tmat.at[t], mstage.at[t], lsem.at[3 + kinds + t])
        for t in range(skinds)
    ]
    for c in loads + tl + [bl] + ml_:
        c.start()

    barrier = pltpu.get_barrier_semaphore()

    partners = [lax.rem(me + 1, n), lax.rem(me + n - 1, n)]
    partners += [near_peer(d) for d in range(1, near)]
    partners += [far_peer(d) for d in range(1, far)]
    for peer in partners:
        pl.semaphore_signal(barrier, inc=1, device_id={"blk": peer}, device_id_type=MESH)
    pl.semaphore_wait(barrier, len(partners))

    def halo_copy(src, halo, step, side, c):
        peer = jnp.minimum(me + 1, n - 1) if side == 0 else jnp.maximum(me - 1, 0)
        at = pl.ds(chunks[c][0], chunks[c][1])
        return pltpu.make_async_remote_copy(
            src_ref=src.at[:, at, :],
            dst_ref=halo.at[side, :, at, :],
            send_sem=hsend.at[step, side, c],
            recv_sem=hrecv.at[step, side, c],
            device_id={"blk": peer},
            device_id_type=MESH,
        )

    def halo_start(src, halo, step, c):
        @pl.when(me < n - 1)
        def _():
            halo_copy(src, halo, step, 0, c).start()

        @pl.when(me > 0)
        def _():
            halo_copy(src, halo, step, 1, c).start()

    def halo_wait(src, halo, step, c):
        @pl.when(me < n - 1)
        def _():
            halo_copy(src, halo, step, 0, c).wait_send()
            halo_copy(src, halo, step, 1, c).wait_recv()

        @pl.when(me > 0)
        def _():
            halo_copy(src, halo, step, 1, c).wait_send()
            halo_copy(src, halo, step, 0, c).wait_recv()

    for c in range(len(chunks)):
        halo_start(basis.at[kry - 1], halo1, 0, c)

    @pl.when(me == 0)
    def _():
        halo1[0] = jnp.zeros(halo1.shape[1:], F32)
        halo2[0] = jnp.zeros(halo2.shape[1:], F32)

    @pl.when(me == n - 1)
    def _():
        halo1[1] = jnp.zeros(halo1.shape[1:], F32)
        halo2[1] = jnp.zeros(halo2.shape[1:], F32)

    tail = (coef // 128) * 128
    for z in (za_hi, za_lo, zb_hi, zb_lo):
        z[...] = jnp.zeros(z.shape, BF16)
    if cpad > coef:
        for z in (sh_ref, sl_ref):
            z[coef:, :] = jnp.zeros((cpad - coef, z.shape[1]), BF16)

    loads[1].wait()
    for t in range(kinds):
        ch, cl = split(cstage[t])
        rct[t, :spb, :spb] = ch
        rct[t, :spb, spb:] = ch
        rct[t, spb:, :spb] = cl
        rct[t, spb:, spb:] = cl

    def prepare(src, hi_ref, lo_ref, count):
        def one(t, _):
            hi, lo = split(src[t])
            if cpad > coef:
                hi_ref[t, :, tail:] = jnp.zeros((coef, cpad - tail), BF16)
                lo_ref[t, :, tail:] = jnp.zeros((coef, cpad - tail), BF16)
            hi_ref[t, :, :coef] = hi
            lo_ref[t, :, :coef] = lo
            return 0

        lax.fori_loop(0, count, one, 0)

    for c in tl:
        c.wait()

    def prepare_pair(u, _):
        for k in range(2):
            for dst, part in zip((thi, tlo), split(stage[2 * u + k])):
                for c, (at, size) in enumerate(chunks):
                    if size < CHUNK:
                        dst[c, u, :, k * CHUNK : (k + 1) * CHUNK] = jnp.zeros((coef, CHUNK), BF16)
                    dst[c, u, :, k * CHUNK : k * CHUNK + size] = part[:, at : at + size]
        return 0

    lax.fori_loop(0, kinds // 2, prepare_pair, 0)
    loads[0].wait()
    bl.wait()

    pairs = [(i, j) for i in range(kry) for j in range(i, kry)]
    groups = coef // 8

    def sums(count, terms, start=0, size=coef, carry=None):
        def row(r, carry):
            at = pl.ds(pl.multiple_of(r * 8, 8), 8)
            for b in range(nb):
                new = terms(b, at)
                carry = tuple(x + y for x, y in zip(carry, new))
            return carry

        if carry is None:
            carry = (jnp.zeros((8, 128), F32),) * count
        return lax.fori_loop(start // 8, (start + size) // 8, row, carry)

    def gram_terms(b, at):
        vs = [bv[i, b, at, :] for i in range(kry)]
        return [vs[i] * vs[j] for i, j in pairs]

    gram = sums(len(pairs), gram_terms)
    gbuf[...] = jnp.concatenate(
        [jnp.sum(g, axis=0, keepdims=True) for g in gram]
        + [jnp.zeros((gbuf.shape[0] - len(pairs), 128), F32)],
        axis=0,
    )
    for c in ml_:
        c.wait()
    prepare(mstage, mhi, mlo, skinds)

    def operator_apply(vec, sent, halo, step):
        def source(p, at, size):
            rows = slice(at, at + size)
            if p < nb:
                return halo[0, p, rows]
            if p < 2 * nb:
                return vec[p - nb, rows]
            return halo[1, p - 2 * nb, rows]

        def couple(c, u, hi_ref, lo_ref):
            at, size = chunks[c]
            for k in range(2):
                t = 2 * u + k
                parts = []
                for b in range(nb):
                    m = None
                    for p in range(nb + b - REACH, nb + b + REACH + 1):
                        term = w_ref[(b * kinds + t) * window + p] * source(p, at, size)
                        m = term if m is None else m + term
                    parts.append(jnp.concatenate(split(m), axis=1))
                r = lax.dot_general(
                    jnp.concatenate(parts, axis=0),
                    rct[t],
                    (((1,), (1,)), ((), ())),
                    preferred_element_type=F32,
                )
                zh, zl = split(r[:, :spb] + r[:, spb:])
                for b in range(nb):
                    to = (slice(k * CHUNK, k * CHUNK + size), slice(b * spb, (b + 1) * spb))
                    hi_ref[to] = zh[b * size : (b + 1) * size]
                    lo_ref[to] = zl[b * size : (b + 1) * size]

        def move(c, u, hi_ref, lo_ref):
            hi = hi_ref[...]
            y = mm(thi[c, u], hi) + mm(thi[c, u], lo_ref[...]) + mm(tlo[c, u], hi)
            if c == 0 and u == 0:
                acc[...] = y
            else:
                acc[...] += y

        bufs = ((za_hi, za_lo), (zb_hi, zb_lo))
        turn = 0
        for c in range(len(chunks)):
            halo_wait(sent, halo, step, c)
            couple(c, 0, *bufs[turn])
            for u in range(kinds // 2):
                if u + 1 < kinds // 2:
                    couple(c, u + 1, *bufs[1 - turn])
                move(c, u, *bufs[turn])
                turn = 1 - turn
        sh, sl = split(acc[...])
        sh_ref[:coef, :] = sh
        sl_ref[:coef, :] = sl
        acc[...] = jnp.concatenate([vec[b] for b in range(nb)], axis=1)
        kind_row = jnp.concatenate([stype[b : b + 1, :] for b in range(nb)], axis=1)

        def scatter(t, _):
            hi = sh_ref[...]
            y = mm(mhi[t], hi) + mm(mhi[t], sl_ref[...]) + mm(mlo[t], hi)
            mask = (kind_row == t).astype(F32)
            acc[...] -= mask * y
            return 0

        lax.fori_loop(0, skinds, scatter, 0)
        for b in range(nb):
            wbuf[b] = acc[:, b * spb : (b + 1) * spb]

    lane = lax.broadcasted_iota(jnp.int32, (8, 128), 1)

    def allreduce(step, rows):
        k = rows.shape[0]
        tot = jnp.sum(rows, axis=1, keepdims=True)
        here = lax.broadcasted_iota(jnp.int32, (k, 128), 1) == lax.broadcasted_iota(
            jnp.int32, (k, 128), 0
        )
        packed = jnp.sum(jnp.where(here, tot, 0.0), axis=0, keepdims=True)
        packed = jnp.broadcast_to(packed, (8, 128))
        total = packed
        for turn, (slots, rs, size, spot, peer_of) in enumerate(
            (
                (slots_a, ra_sem, near, my_near, near_peer),
                (slots_b, rb_sem, far, my_far, far_peer),
            )
        ):
            send[step, turn] = total
            slots[step, spot] = total

            def copy(d, slot):
                return pltpu.make_async_remote_copy(
                    src_ref=send.at[step, turn],
                    dst_ref=slots.at[step, slot],
                    send_sem=ssem.at[step, turn, d],
                    recv_sem=rs.at[step, slot],
                    device_id={"blk": peer_of(d)},
                    device_id_type=MESH,
                )

            for d in range(1, size):
                copy(d, spot).start()
            for d in range(1, size):
                c = copy(d, lax.rem(spot + d, size))
                c.wait_send()
                c.wait_recv()
            total = jnp.sum(slots[step], axis=0)
        return lambda i: jnp.sum(jnp.where(lane == i, total, 0.0), axis=1, keepdims=True)

    def pack(parts, more):
        rows = [jnp.sum(x, axis=0, keepdims=True) for x in parts]
        pad = (-len(rows)) % 8
        rows += [jnp.zeros((1, 128), F32)] * pad
        head = jnp.concatenate(rows, axis=0)
        return (head if more is None else jnp.concatenate([head, more], axis=0)), len(rows)

    def norm(count, proj, image_sq, gram_of):
        coeffs = [x / cells for x in proj]
        squares = image_sq
        for i in range(count):
            inner = None
            for j in range(count):
                term = gram_of(i, j) * coeffs[j]
                inner = term if inner is None else inner + term
            squares = squares + coeffs[i] * (inner - 2.0 * proj[i])
        return coeffs, jnp.sqrt(squares / cells + 1e-06)

    def hess_row(coeffs, beta):
        row = jnp.zeros((8, 128), F32)
        for i, c in enumerate(coeffs + [beta]):
            row = jnp.where(lane == i, c, row)
        return row

    operator_apply(bv.at[kry - 1], basis.at[kry - 1], halo1, 0)

    def proj_terms1(b, at):
        w = wbuf[b, at, :]
        return [w * bv[i, b, at, :] for i in range(kry)] + [w * w]

    rows, base = pack(sums(kry + 1, proj_terms1), gbuf[...])
    get1 = allreduce(0, rows)
    gram8 = {}
    for k, (i, j) in enumerate(pairs):
        gram8[i, j] = gram8[j, i] = get1(base + k)
    h1, beta1 = norm(kry, [get1(i) for i in range(kry)], get1(kry), lambda i, j: gram8[i, j])
    hess[0] = hess_row(h1, beta1)
    inv1 = 1.0 / beta1

    def first_terms(b, at):
        f = wbuf[b, at, :]
        vs = [bv[i, b, at, :] for i in range(kry)]
        for i in range(kry):
            f = f - h1[i] * vs[i]
        f = f * inv1
        fbuf[0, b, at, :] = f
        return [f * v for v in vs] + [f * f]

    extra = None
    for c, (at, size) in enumerate(chunks):
        extra = sums(kry + 1, first_terms, at, size, extra)
        halo_start(fbuf.at[0], halo2, 1, c)
    first_out = pltpu.make_async_copy(fbuf.at[0], out.at[0], osem.at[0])
    first_out.start()

    operator_apply(fbuf.at[0], fbuf.at[0], halo2, 1)

    def proj_terms2(b, at):
        w = wbuf[b, at, :]
        return [w * bv[i, b, at, :] for i in range(kry)] + [w * fbuf[0, b, at, :], w * w]

    rows, _ = pack(tuple(sums(kry + 2, proj_terms2)) + tuple(extra), None)
    get2 = allreduce(1, rows)
    gram9 = dict(gram8)
    for i in range(kry + 1):
        gram9[i, kry] = gram9[kry, i] = get2(kry + 2 + i)
    h2, beta2 = norm(
        kry + 1, [get2(i) for i in range(kry + 1)], get2(kry + 1), lambda i, j: gram9[i, j]
    )
    hess[1] = hess_row(h2, beta2)
    inv2 = 1.0 / beta2

    def second(r, _):
        at = pl.ds(pl.multiple_of(r * 8, 8), 8)
        for b in range(nb):
            f = wbuf[b, at, :]
            for i in range(kry):
                f = f - h2[i] * bv[i, b, at, :]
            f = f - h2[kry] * fbuf[0, b, at, :]
            fbuf[1, b, at, :] = f * inv2
        return 0

    lax.fori_loop(0, groups, second, 0)
    second_out = pltpu.make_async_copy(fbuf.at[1], out.at[1], osem.at[1])
    second_out.start()
    first_out.wait()
    second_out.wait()


def shards(n, basis, nbr_block, nbr_type, nbr_count, sphere_type, trans, coup, tmat):
    kry, nb, coef, spb = basis.shape
    kinds, skinds = trans.shape[0], tmat.shape[0]
    cpad = -(-coef // 128) * 128
    window = 3 * nb
    rows = nbr_block - lax.axis_index("blk") * nb + nb
    live = jnp.arange(nbr_block.shape[1], dtype=jnp.int32)[None, :] < nbr_count[:, None]
    code = jnp.where(live, nbr_type * window + rows, -1)
    weights = jnp.sum(
        (code[:, None, :] == jnp.arange(kinds * window, dtype=jnp.int32)[None, :, None]).astype(F32),
        axis=2,
    ).reshape(-1)
    npairs = kry * (kry + 1) // 2
    any_ = pl.BlockSpec(memory_space=pl.ANY)
    vm = pl.BlockSpec(memory_space=pltpu.VMEM)
    wide = nb * spb
    nch = -(-coef // CHUNK)
    near, far = factors(n)
    out, hess = pl.pallas_call(
        functools.partial(kernel, n, (kry, nb, coef, spb, kinds, skinds, cpad)),
        out_shape=(
            jax.ShapeDtypeStruct((2, nb, coef, spb), F32),
            jax.ShapeDtypeStruct((2, 8, 128), F32),
        ),
        in_specs=[pl.BlockSpec(memory_space=pltpu.SMEM), vm, any_, any_, any_, any_],
        out_specs=(any_, vm),
        scratch_shapes=[
            pltpu.VMEM((kry, nb, coef, spb), F32),
            pltpu.VMEM((kinds, coef, coef), F32),
            pltpu.VMEM((skinds, coef, coef), F32),
            pltpu.VMEM((kinds, spb, spb), F32),
            pltpu.VMEM((nch, kinds // 2, coef, 2 * CHUNK), BF16),
            pltpu.VMEM((nch, kinds // 2, coef, 2 * CHUNK), BF16),
            pltpu.VMEM((skinds, coef, cpad), BF16),
            pltpu.VMEM((skinds, coef, cpad), BF16),
            pltpu.VMEM((kinds, 2 * spb, 2 * spb), BF16),
            pltpu.VMEM((2, nb, coef, spb), F32),
            pltpu.VMEM((2, nb, coef, spb), F32),
        ]
        + [pltpu.VMEM((2 * CHUNK, wide), BF16)] * 4
        + [pltpu.VMEM((cpad, wide), BF16)] * 2
        + [
            pltpu.VMEM((coef, wide), F32),
            pltpu.VMEM((nb, coef, spb), F32),
            pltpu.VMEM((2, nb, coef, spb), F32),
            pltpu.VMEM((-(-npairs // 8) * 8, 128), F32),
            pltpu.VMEM((2, 2, 8, 128), F32),
            pltpu.VMEM((2, near, 8, 128), F32),
            pltpu.VMEM((2, far, 8, 128), F32),
            pltpu.SemaphoreType.DMA((3 + kinds + skinds,)),
            pltpu.SemaphoreType.DMA((2, 2, max(near, far))),
            pltpu.SemaphoreType.DMA((2, near)),
            pltpu.SemaphoreType.DMA((2, far)),
            pltpu.SemaphoreType.DMA((2, 2, nch)),
            pltpu.SemaphoreType.DMA((2, 2, nch)),
            pltpu.SemaphoreType.DMA((2,)),
        ],
        compiler_params=pltpu.CompilerParams(
            collective_id=0, has_side_effects=True, vmem_limit_bytes=60 * 1024 * 1024
        ),
    )(weights, sphere_type, basis, trans, coup, tmat)
    return out, hess[0, 0, : kry + 1], hess[1, 0, : kry + 2]


def solution(mesh):
    return jax.shard_map(
        functools.partial(shards, mesh.shape["blk"]),
        mesh=mesh,
        in_specs=(
            P(None, ("groups", "blk"), None, None),
            P(("groups", "blk"), None),
            P(("groups", "blk"), None),
            P(("groups", "blk")),
            P(("groups", "blk"), None),
            P(),
            P(),
            P(),
        ),
        out_specs=(P(None, ("groups", "blk"), None, None), P("groups"), P("groups")),
        check_vma=False,
    )
```
